32 devices in a mesh: dp: 4 (over x, y), ep: 8 (over z, core).
Axes of the slice: x: 2, y: 2, z: 4, core: 2. Of those that a mesh axis runs over, the one named last changes fastest.
Arguments:
- x: bfloat16 [4, 8, 256, 3072], P('dp', 'ep'), parts along dimension 0
- expert: int32 [4, 8, 256, 2], P('dp', 'ep'), parts along dimension 0
- slot: int32 [4, 8, 256, 2], P('dp', 'ep'), parts along dimension 0
- gate: float32 [4, 8, 256, 2], P('dp', 'ep'), parts along dimension 0
- w_gate: bfloat16 [8, 3072, 16384], P('ep')
- w_up: bfloat16 [8, 3072, 16384], P('ep')
- w_down: bfloat16 [8, 16384, 3072], P('ep')
Outputs:
- y: bfloat16 [4, 8, 256, 3072], P('dp', 'ep'), parts along dimension 0
There are 4 independent parts. The reference program is written for one: setup_inputs(seed, part) draws one part's arguments, and reference() takes and returns one part's arrays. A program takes and returns all parts, laid end to end along the dimension named above; an argument that names none is the same for every part.
All inputs are finite; a program needn't handle non-finite values.
Results may differ from the reference program's by a relative error of at most 0.009.
Values are sent between devices in bfloat16 or wider.
A program may use at most 2 GiB of HBM per device.

```python
import jax
import jax.numpy as jnp

MEMBERS = 8
TOKENS = 256
D = 3072
FF = 16384
TOP = 2
EXPERTS = 8
SLOTS = 5 * TOKENS * TOP // (4 * EXPERTS)


def setup_inputs(seed: int = 0, part: int = 0) -> dict:
    own, k1, k2, k3, k4, k5, k6 = jax.random.split(jax.random.key(seed), 7)
    kx, ke, kl, kg = jax.random.split(jax.random.fold_in(own, part), 4)
    devices = (1, MEMBERS)
    place = jax.random.permutation(kl, jnp.arange(EXPERTS, dtype=jnp.uint32))
    slow = ((EXPERTS + (9 * place) % EXPERTS) << ((9 * place) // EXPERTS)) // EXPERTS
    wait = (jax.random.bits(ke, (*devices, TOKENS, EXPERTS), jnp.uint32) >> 10) * slow
    expert = jnp.argsort(wait, axis=-1)[..., :TOP].astype(jnp.int32)
    chosen = jax.nn.one_hot(expert, EXPERTS, dtype=jnp.int32)
    in_line = jnp.cumsum(chosen.reshape(*devices, TOKENS * TOP, EXPERTS), axis=2) - 1
    slot = jnp.sum(in_line.reshape(chosen.shape) * chosen, axis=-1)

    def one(key, rows, columns):
        return (jax.random.normal(key, (rows, columns), jnp.float32) * rows**-0.5).astype(jnp.bfloat16)

    def weights(key, rows, columns):
        return jax.lax.map(lambda k: one(k, rows, columns), jax.random.split(key, EXPERTS))

    return {
        "x": jax.random.normal(kx, (*devices, TOKENS, D), jnp.float32).astype(jnp.bfloat16),
        "expert": expert,
        "slot": slot,
        "gate": jax.nn.softmax(jax.random.normal(kg, expert.shape, jnp.float32)),
        "w_gate": weights(k1, D, FF),
        "w_up": weights(k2, D, FF),
        "w_down": weights(k3, FF, D),
    }


def einsum(form, a, b):
    return jnp.einsum(form, a.astype(jnp.float32), b.astype(jnp.float32))


def reference(x, expert, slot, gate, w_gate, w_up, w_down):
    to_expert = jax.nn.one_hot(expert, EXPERTS, dtype=jnp.bfloat16)
    to_slot = jax.nn.one_hot(slot, SLOTS, dtype=jnp.bfloat16)
    weighted = to_expert * gate[..., None].astype(jnp.bfloat16)
    dispatch = einsum("abtke,abtkc->abtec", to_expert, to_slot).astype(jnp.bfloat16)
    combine = einsum("abtke,abtkc->abtec", weighted, to_slot).astype(jnp.bfloat16)
    z = einsum("abtec,abtd->aebcd", dispatch, x).astype(jnp.bfloat16)
    h = jax.nn.silu(einsum("aebcd,edf->aebcf", z, w_gate))
    h = (h * einsum("aebcd,edf->aebcf", z, w_up)).astype(jnp.bfloat16)
    out = einsum("aebcf,efd->aebcd", h, w_down).astype(jnp.bfloat16)
    y = einsum("abtec,aebcd->abtd", combine, out)
    return y.astype(jnp.bfloat16)
```

```python
import functools

import jax
import jax.numpy as jnp
from jax import lax
from jax.experimental import pallas as pl
from jax.experimental.pallas import tpu as pltpu
from jax.sharding import PartitionSpec as P

MESH = pl.DeviceIdType.MESH
TF = 256
TD = 256
GB = 4
DB = 4
KB = 4


def flipped(me, r):
    bits = [me % 2, (me // 2) % 2, me // 4]
    return sum(((1 - b) if (r >> i) & 1 else b) * (1 << i) for i, b in enumerate(bits))


def kernel(
    z_ref, wg_ref, wu_ref, wd_ref, wc_ref, y_ref,
    zbuf, h, osend, orecv, wgb, wub, wdb, g0, g1, u0, u1, acc, ybuf,
    wg_sem, wu_sem, wd_sem, zs_sem, zr_sem, os_sem, or_sem, own_sem, y_sem,
):
    members, slots, d = z_ref.shape
    ff = wg_ref.shape[1]
    rows = members * slots
    half = rows // 2
    tiles, chunks, kd = ff // TF, d // TD, ff // KB
    me = lax.axis_index("ep")
    peer = [flipped(me, r) for r in range(members)]

    def fetch_g(i):
        tile, b = i % tiles, i % GB
        cols = pl.ds(pl.multiple_of(tile * TF, TF), TF)
        return (
            pltpu.make_async_copy(wg_ref.at[:, cols], wgb.at[b], wg_sem.at[b]),
            pltpu.make_async_copy(wu_ref.at[:, cols], wub.at[b], wu_sem.at[b]),
        )

    def fetch_d(i):
        c, k, b = i // KB, i % KB, i % DB
        cols = pl.ds(pl.multiple_of(c * TD, TD), TD)
        deep = pl.ds(pl.multiple_of(k * kd, kd), kd)
        return pltpu.make_async_copy(wd_ref.at[deep, cols], wdb.at[b], wd_sem.at[b])

    def begin(copies):
        for c in copies:
            c.start()

    for i in range(GB - 1):
        begin(fetch_g(i))

    barrier = pltpu.get_barrier_semaphore()
    for r in range(1, members):
        pl.semaphore_signal(barrier, inc=1, device_id={"ep": peer[r]}, device_id_type=MESH)
    own = pltpu.make_async_copy(z_ref.at[0], zbuf.at[pl.ds(0, slots)], own_sem)
    own.start()
    pl.semaphore_wait(barrier, members - 1)

    def send_z(r):
        return pltpu.make_async_remote_copy(
            src_ref=z_ref.at[r],
            dst_ref=zbuf.at[pl.ds(r * slots, slots)],
            send_sem=zs_sem.at[r],
            recv_sem=zr_sem.at[r],
            device_id={"ep": peer[r]},
            device_id_type=MESH,
        )

    order = [2, 3, 1, 6, 7, 4, 5]
    for r in order:
        send_z(r).start()

    def gate_up(first, base):
        gs, us = (g0, g1), (u0, u1)

        def activate(step, p):
            cols = pl.ds(pl.multiple_of(step * TF, TF), TF)
            h[pl.ds(base, half), cols] = (jax.nn.silu(gs[p][...]) * us[p][...]).astype(h.dtype)

        def one(i, p, last):
            @pl.when(i + GB - 1 < last)
            def _():
                begin(fetch_g(i + GB - 1))

            for c in fetch_g(i):
                c.wait()
            b = i % GB
            z = zbuf[pl.ds(base, half), :]
            activate(lax.max(i - first - 1, 0), 1 - p)
            gs[p][...] = jnp.dot(z, wgb[b], preferred_element_type=jnp.float32)
            us[p][...] = jnp.dot(z, wub[b], preferred_element_type=jnp.float32)

        def pair(j, _):
            one(first + 2 * j, 0, 2 * tiles)
            one(first + 2 * j + 1, 1, 2 * tiles)
            return 0

        lax.fori_loop(0, tiles // 2, pair, 0)
        activate(tiles - 1, 1)

    g1[...] = jnp.zeros_like(g1)
    u1[...] = jnp.zeros_like(u1)

    own.wait()
    for r in range(1, members // 2):
        send_z(r).wait_recv()
    gate_up(0, 0)
    for i in range(DB - 1):
        fetch_d(i).start()
    for r in range(members // 2, members):
        send_z(r).wait_recv()
    gate_up(tiles, half)

    def send_o(c, r):
        return pltpu.make_async_remote_copy(
            src_ref=osend.at[c, pl.ds(r * slots, slots)],
            dst_ref=orecv.at[c, pl.ds(r * slots, slots)],
            send_sem=os_sem.at[c, r],
            recv_sem=or_sem.at[c, r],
            device_id={"ep": peer[r]},
            device_id_type=MESH,
        )

    def send_chunk(c):
        for r in (6, 7, 4, 5, 2, 3, 1):
            send_o(c, r).start()

    def down(c, _):
        for k in range(KB):
            i = c * KB + k

            @pl.when(i + DB - 1 < chunks * KB)
            def _():
                fetch_d(i + DB - 1).start()

            fetch_d(i).wait()
            part = jnp.dot(h[:, k * kd:(k + 1) * kd], wdb[i % DB], preferred_element_type=jnp.float32)
            if k == 0:
                acc[...] = part

                @pl.when(c > 0)
                def _():
                    send_chunk(c - 1)
            elif k < KB - 1:
                acc[...] += part
            else:
                out = (acc[...] + part).astype(osend.dtype)
                osend[c] = out
                orecv[c, pl.ds(0, slots), :] = out[:slots]
        return 0

    lax.fori_loop(0, chunks, down, 0)
    send_chunk(chunks - 1)

    def put_y(c):
        cols = pl.ds(pl.multiple_of(c * TD, TD), TD)
        return pltpu.make_async_copy(ybuf.at[c], y_ref.at[:, cols], y_sem.at[c])

    def combine(c, _):
        for r in range(1, members):
            send_o(c, r).wait_recv()
        ybuf[c] = jnp.dot(wc_ref[...], orecv[c], preferred_element_type=jnp.float32).astype(ybuf.dtype)
        put_y(c).start()
        return 0

    lax.fori_loop(0, chunks, combine, 0)

    def drain(c, _):
        for r in range(1, members):
            send_o(c, r).wait_send()
        put_y(c).wait()
        return 0

    for r in range(1, members):
        send_z(r).wait_send()
    lax.fori_loop(0, chunks, drain, 0)


def experts(z, wg, wu, wd, wc):
    members, slots, d = z.shape
    ff, tokens = wg.shape[1], wc.shape[0]
    rows, chunks = members * slots, d // TD
    bf16, f32 = jnp.bfloat16, jnp.float32
    dma = pltpu.SemaphoreType.DMA
    hbm = pl.BlockSpec(memory_space=pl.ANY)
    half = rows // 2
    return pl.pallas_call(
        kernel,
        out_shape=jax.ShapeDtypeStruct((tokens, d), bf16),
        in_specs=[hbm, hbm, hbm, hbm, pl.BlockSpec(memory_space=pltpu.VMEM)],
        out_specs=hbm,
        scratch_shapes=[
            pltpu.VMEM((rows, d), bf16),
            pltpu.VMEM((rows, ff), bf16),
            pltpu.VMEM((chunks, rows, TD), bf16),
            pltpu.VMEM((chunks, rows, TD), bf16),
            pltpu.VMEM((GB, d, TF), bf16),
            pltpu.VMEM((GB, d, TF), bf16),
            pltpu.VMEM((DB, ff // KB, TD), bf16),
            pltpu.VMEM((half, TF), f32),
            pltpu.VMEM((half, TF), f32),
            pltpu.VMEM((half, TF), f32),
            pltpu.VMEM((half, TF), f32),
            pltpu.VMEM((rows, TD), f32),
            pltpu.VMEM((chunks, tokens, TD), bf16),
            dma((GB,)), dma((GB,)), dma((DB,)),
            dma((members,)), dma((members,)),
            dma((chunks, members)), dma((chunks, members)),
            dma, dma((chunks,)),
        ],
        compiler_params=pltpu.CompilerParams(
            collective_id=0, has_side_effects=True, vmem_limit_bytes=66_000_000
        ),
        cost_estimate=pl.CostEstimate(
            flops=6 * rows * d * ff, bytes_accessed=6 * d * ff, transcendentals=rows * ff
        ),
    )(z, wg, wu, wd, wc)


def solution(mesh):
    def step(x, expert, slot, gate, wg, wu, wd):
        x, expert, slot, gate = x[0, 0], expert[0, 0], slot[0, 0], gate[0, 0]
        tokens, top = expert.shape
        members = mesh.shape["ep"]
        slots = 5 * tokens * top // (4 * members)
        me = lax.axis_index("ep")
        relative = jnp.bitwise_xor(expert, me)
        to_expert = jax.nn.one_hot(relative, members, dtype=jnp.bfloat16)
        to_slot = jax.nn.one_hot(slot, slots, dtype=jnp.bfloat16)
        weighted = to_expert * gate[..., None].astype(jnp.bfloat16)
        f32 = jnp.float32
        dispatch = jnp.einsum("tke,tkc->ect", to_expert.astype(f32), to_slot.astype(f32)).astype(jnp.bfloat16)
        combine = jnp.einsum("tke,tkc->tec", weighted.astype(f32), to_slot.astype(f32)).astype(jnp.bfloat16)
        z = jnp.einsum("ect,td->ecd", dispatch.astype(f32), x.astype(f32)).astype(jnp.bfloat16)
        y = experts(z, wg[0], wu[0], wd[0], combine.reshape(tokens, members * slots))
        return y[None, None]

    tok, exp = P("dp", "ep"), P("ep")
    return jax.shard_map(
        step, mesh=mesh, in_specs=(tok, tok, tok, tok, exp, exp, exp), out_specs=tok, check_vma=False
    )
```

```python
import functools

import jax
import jax.numpy as jnp
from jax import lax
from jax.experimental import pallas as pl
from jax.experimental.pallas import tpu as pltpu
from jax.sharding import PartitionSpec as P

MESH = pl.DeviceIdType.MESH
TF = 512
TD = 256
GB = 3
DB = 3
KB = 4


def flipped(me, r):
    bits = [me % 2, (me // 2) % 2, me // 4]
    return sum(((1 - b) if (r >> i) & 1 else b) * (1 << i) for i, b in enumerate(bits))


def kernel(
    members,
    x_ref, expert_ref, slot_ref, gate_ref, wg_ref, wu_ref, wd_ref, y_ref,
    zbuf, h, osend, orecv, wgb, wub, wdb, acc0, acc1, ybuf, wc,
    wg_sem, wu_sem, wd_sem, zs_sem, zr_sem, os_sem, or_sem, x_sem, y_sem,
):
    tokens, d = x_ref.shape
    ff = wg_ref.shape[1]
    rows = zbuf.shape[0]
    slots = rows // members
    half = rows // 2
    tiles, chunks, kd = ff // TF, d // TD, ff // KB
    me = lax.axis_index("ep")
    peer = [flipped(me, r) for r in range(members)]

    def fetch_g(i):
        tile, b = i % tiles, i % GB
        cols = pl.ds(pl.multiple_of(tile * TF, TF), TF)
        return (
            pltpu.make_async_copy(wg_ref.at[:, cols], wgb.at[b], wg_sem.at[b]),
            pltpu.make_async_copy(wu_ref.at[:, cols], wub.at[b], wu_sem.at[b]),
        )

    def fetch_d(i):
        c, k, b = i // KB, i % KB, i % DB
        cols = pl.ds(pl.multiple_of(c * TD, TD), TD)
        deep = pl.ds(pl.multiple_of(k * kd, kd), kd)
        return pltpu.make_async_copy(wd_ref.at[deep, cols], wdb.at[b], wd_sem.at[b])

    def begin(copies):
        for c in copies:
            c.start()

    load_x = pltpu.make_async_copy(x_ref, ybuf, x_sem)
    load_x.start()
    for i in range(GB - 1):
        begin(fetch_g(i))

    barrier = pltpu.get_barrier_semaphore()
    for r in range(1, members):
        pl.semaphore_signal(barrier, inc=1, device_id={"ep": peer[r]}, device_id_type=MESH)
    place = [
        jnp.where(slot_ref[j:j + 1, :] < slots, expert_ref[j:j + 1, :] * slots + slot_ref[j:j + 1, :], -1)
        for j in range(expert_ref.shape[0])
    ]
    line = lax.broadcasted_iota(jnp.int32, (slots, tokens), 0)

    def chosen(r, values):
        here = line + peer[r] * slots
        return sum(jnp.where(here == p, v, 0.0) for p, v in zip(place, values))

    def rows_of(r):
        pick = chosen(r, [1.0] * len(place)).astype(x_ref.dtype)
        return jnp.dot(pick, ybuf[...], preferred_element_type=jnp.float32).astype(zbuf.dtype)

    def send_z(r):
        return pltpu.make_async_remote_copy(
            src_ref=osend.at[pl.ds(r * slots, slots)],
            dst_ref=zbuf.at[pl.ds(r * slots, slots)],
            send_sem=zs_sem.at[r],
            recv_sem=zr_sem.at[r],
            device_id={"ep": peer[r]},
            device_id_type=MESH,
        )

    load_x.wait()
    pl.semaphore_wait(barrier, members - 1)
    groups = [(2, 3), (6, 7), (4, 5), (1, 0)]
    for now, before in zip(groups + [()], [()] + groups):
        for r in now:
            if r == 0:
                zbuf[0:slots, :] = rows_of(r)
            else:
                osend[r * slots:(r + 1) * slots, :] = rows_of(r)
        for r in before:
            if r > 0:
                send_z(r).start()

    weights = [gate_ref[j:j + 1, :].astype(wc.dtype).astype(jnp.float32) for j in range(len(place))]
    table = jnp.concatenate([chosen(r, weights) for r in range(members)], axis=0)
    wc[...] = table.T.astype(wc.dtype)

    def gate_up(first, base):
        def one(j, _):
            i = first + j

            @pl.when(i + GB - 1 < 2 * tiles)
            def _():
                begin(fetch_g(i + GB - 1))

            for c in fetch_g(i):
                c.wait()
            b = i % GB
            z = zbuf[pl.ds(base, half), :]
            g = jnp.dot(z, wgb[b], preferred_element_type=jnp.float32)
            u = jnp.dot(z, wub[b], preferred_element_type=jnp.float32)
            cols = pl.ds(pl.multiple_of(j * TF, TF), TF)
            h[pl.ds(base, half), cols] = (jax.nn.silu(g) * u).astype(h.dtype)
            return 0

        lax.fori_loop(0, tiles, one, 0)

    for r in range(1, members // 2):
        send_z(r).wait_recv()
    gate_up(0, 0)
    for i in range(DB - 1):
        fetch_d(i).start()
    for r in range(members // 2, members):
        send_z(r).wait_recv()
    gate_up(tiles, half)
    for r in range(1, members):
        send_z(r).wait_send()

    def chunk(c):
        return pl.ds(pl.multiple_of(c * TD, TD), TD)

    def send_o(c, r):
        return pltpu.make_async_remote_copy(
            src_ref=osend.at[pl.ds(r * slots, slots), chunk(c)],
            dst_ref=orecv.at[pl.ds(r * slots, slots), chunk(c)],
            send_sem=os_sem.at[c, r],
            recv_sem=or_sem.at[c, r],
            device_id={"ep": peer[r]},
            device_id_type=MESH,
        )

    def send_chunk(c):
        for r in (6, 7, 4, 5, 2, 3, 1):
            send_o(c, r).start()

    def down(c, _):
        for k in range(KB):
            i = c * KB + k

            @pl.when(i + DB - 1 < chunks * KB)
            def _():
                fetch_d(i + DB - 1).start()

            fetch_d(i).wait()
            w = wdb[i % DB]
            for s, acc in enumerate((acc0, acc1)):
                deep = h[s * half:(s + 1) * half, k * kd:(k + 1) * kd]
                part = jnp.dot(deep, w, preferred_element_type=jnp.float32)
                if k == 0:
                    acc[...] = part
                elif k < KB - 1:
                    acc[...] += part
                else:
                    out = (acc[...] + part).astype(osend.dtype)
                    osend[pl.ds(s * half, half), chunk(c)] = out
                    if s == 0:
                        orecv[pl.ds(0, slots), chunk(c)] = out[:slots]
            if k == 0:

                @pl.when(c > 0)
                def _():
                    send_chunk(c - 1)

        return 0

    lax.fori_loop(0, chunks, down, 0)
    send_chunk(chunks - 1)

    def put_y(c):
        return pltpu.make_async_copy(ybuf.at[:, chunk(c)], y_ref.at[:, chunk(c)], y_sem.at[c])

    def combine(c, _):
        for r in range(1, members):
            send_o(c, r).wait_recv()
        ybuf[:, chunk(c)] = jnp.dot(
            wc[...], orecv[:, chunk(c)], preferred_element_type=jnp.float32
        ).astype(ybuf.dtype)
        put_y(c).start()
        return 0

    lax.fori_loop(0, chunks, combine, 0)

    def drain(c, _):
        for r in range(1, members):
            send_o(c, r).wait_send()
        put_y(c).wait()
        return 0

    lax.fori_loop(0, chunks, drain, 0)


def experts(members, slots, x, expert, slot, gate, wg, wu, wd):
    tokens, d = x.shape
    ff = wg.shape[1]
    rows, chunks = members * slots, d // TD
    bf16, f32 = jnp.bfloat16, jnp.float32
    dma = pltpu.SemaphoreType.DMA
    hbm = pl.BlockSpec(memory_space=pl.ANY)
    vmem = pl.BlockSpec(memory_space=pltpu.VMEM)
    half = rows // 2
    return pl.pallas_call(
        functools.partial(kernel, members),
        out_shape=jax.ShapeDtypeStruct((tokens, d), bf16),
        in_specs=[hbm, vmem, vmem, vmem, hbm, hbm, hbm],
        out_specs=hbm,
        scratch_shapes=[
            pltpu.VMEM((rows, d), bf16),
            pltpu.VMEM((rows, ff), bf16),
            pltpu.VMEM((rows, d), bf16),
            pltpu.VMEM((rows, d), bf16),
            pltpu.VMEM((GB, d, TF), bf16),
            pltpu.VMEM((GB, d, TF), bf16),
            pltpu.VMEM((DB, ff // KB, TD), bf16),
            pltpu.VMEM((half, TD), f32),
            pltpu.VMEM((half, TD), f32),
            pltpu.VMEM((tokens, d), bf16),
            pltpu.VMEM((tokens, rows), bf16),
            dma((GB,)), dma((GB,)), dma((DB,)),
            dma((members,)), dma((members,)),
            dma((chunks, members)), dma((chunks, members)),
            dma, dma((chunks,)),
        ],
        compiler_params=pltpu.CompilerParams(
            collective_id=0, has_side_effects=True, vmem_limit_bytes=67_000_000
        ),
        cost_estimate=pl.CostEstimate(
            flops=6 * rows * d * ff, bytes_accessed=6 * d * ff, transcendentals=rows * ff
        ),
    )(x, expert, slot, gate, wg, wu, wd)


def solution(mesh):
    def step(x, expert, slot, gate, wg, wu, wd):
        tokens, top = expert.shape[2:]
        members = mesh.shape["ep"]
        slots = 5 * tokens * top // (4 * members)
        y = experts(
            members, slots, x[0, 0], expert[0, 0].T, slot[0, 0].T, gate[0, 0].T, wg[0], wu[0], wd[0]
        )
        return y[None, None]

    tok, exp = P("dp", "ep"), P("ep")
    return jax.shard_map(
        step, mesh=mesh, in_specs=(tok, tok, tok, tok, exp, exp, exp), out_specs=tok, check_vma=False
    )
```
